8 devices in a mesh: dp: 1 (over z), stage: 8 (over y, x, core).
Axes of the slice: x: 2, y: 2, z: 1, core: 2. Of those that a mesh axis runs over, the one named last changes fastest.
Arguments:
- tokens_in: bfloat16 [4, 1024, 1280], P('dp')
- targets: bfloat16 [4, 1024, 1280], P('dp')
- w_in: bfloat16 [16, 1280, 5120], P('stage')
- w_out: bfloat16 [16, 5120, 1280], P('stage')
- norm_gains: float32 [16, 1280], P('stage')
Outputs:
- output 1: float32 [16, 1280, 5120], P(('dp', 'stage'))
- output 2: float32 [16, 5120, 1280], P(('dp', 'stage'))
- output 3: float32 [16, 1280], P(('dp', 'stage'))
- output 4: float32 [1], P('dp')
All inputs are finite; a program needn't handle non-finite values.
Results may differ from the reference program's by a relative error of at most 0.00522216.
Values are sent between devices in bfloat16 or wider.
A program may use at most 1 GiB of HBM per device.

```python
import jax
import jax.numpy as jnp
from jax import lax

STAGES = 8
SEGMENT_LAYERS = 1
MICRO_BATCHES = 4
MICRO_TOKENS = 1024
D_MODEL = 1280
D_FF = 5120
LAYERS = 2 * STAGES * SEGMENT_LAYERS
EPSILON = 1e-6


def setup_inputs(seed: int = 0, part: int = 0) -> dict:
    base_key = jax.random.key(seed)
    key_list = jax.random.split(base_key, 4)
    data_key = jax.random.fold_in(key_list[0], part)
    key_tokens, key_targets = jax.random.split(data_key)
    shape_act = (MICRO_BATCHES, MICRO_TOKENS, D_MODEL)
    target_scale = (1.0 + 0.5 * LAYERS) ** 0.5
    tokens_in = jax.random.normal(key_tokens, shape_act, jnp.float32)
    targets = target_scale * jax.random.normal(key_targets, shape_act, jnp.float32)
    w_in = jax.random.normal(key_list[1], (LAYERS, D_MODEL, D_FF), jnp.float32) * D_MODEL ** -0.5
    w_out = jax.random.normal(key_list[2], (LAYERS, D_FF, D_MODEL), jnp.float32) * D_FF ** -0.5
    norm_gains = 1.0 + 0.5 * jax.random.normal(key_list[3], (LAYERS, D_MODEL), jnp.float32)
    return {
        'tokens_in': tokens_in.astype(jnp.bfloat16),
        'targets': targets.astype(jnp.bfloat16),
        'w_in': w_in.astype(jnp.bfloat16),
        'w_out': w_out.astype(jnp.bfloat16),
        'norm_gains': norm_gains,
    }


def norm_scale(x_f32, gain_vec):
    inv_rms = lax.rsqrt(jnp.mean(x_f32 * x_f32, axis=-1, keepdims=True) + EPSILON)
    return x_f32 * inv_rms * gain_vec


def layer_forward(x_act, first_w, second_w, gain_vec):
    x_f32 = x_act.astype(jnp.float32)
    normed = norm_scale(x_f32, gain_vec).astype(jnp.bfloat16)
    pre_act = jnp.dot(normed, first_w, preferred_element_type=jnp.float32)
    hidden = jax.nn.gelu(pre_act).astype(jnp.bfloat16)
    out_f32 = jnp.dot(hidden, second_w, preferred_element_type=jnp.float32)
    return (x_f32 + out_f32).astype(jnp.bfloat16)


def layer_backward(x_act, grad_h, first_w, second_w, gain_vec):
    x_f32 = x_act.astype(jnp.float32)
    normed_f32, norm_vjp = jax.vjp(norm_scale, x_f32, gain_vec)
    normed = normed_f32.astype(jnp.bfloat16)
    pre_act = jnp.dot(normed, first_w, preferred_element_type=jnp.float32)
    hidden_f32, gelu_vjp = jax.vjp(jax.nn.gelu, pre_act)
    hidden = hidden_f32.astype(jnp.bfloat16)
    grad_second = jnp.dot(hidden.T, grad_h, preferred_element_type=jnp.float32)
    grad_hidden = jnp.dot(grad_h, second_w.T, preferred_element_type=jnp.float32)
    grad_pre = gelu_vjp(grad_hidden)[0].astype(jnp.bfloat16)
    grad_first = jnp.dot(normed.T, grad_pre, preferred_element_type=jnp.float32)
    grad_normed = jnp.dot(grad_pre, first_w.T, preferred_element_type=jnp.float32)
    grad_x_norm, grad_gain = norm_vjp(grad_normed)
    grad_x = (grad_h.astype(jnp.float32) + grad_x_norm).astype(jnp.bfloat16)
    return grad_x, grad_first, grad_second, grad_gain


def to_exec_order(stored):
    tail_shape = stored.shape[1:]
    blocks = stored.reshape((STAGES, 2, SEGMENT_LAYERS) + tail_shape)
    down_half = blocks[:, 0].reshape((STAGES * SEGMENT_LAYERS,) + tail_shape)
    up_half = blocks[::-1, 1].reshape((STAGES * SEGMENT_LAYERS,) + tail_shape)
    return jnp.concatenate([down_half, up_half], axis=0)


def to_stored_order(in_exec):
    tail_shape = in_exec.shape[1:]
    half_rows = STAGES * SEGMENT_LAYERS
    down_half = in_exec[:half_rows].reshape((STAGES, SEGMENT_LAYERS) + tail_shape)
    up_half = in_exec[half_rows:].reshape((STAGES, SEGMENT_LAYERS) + tail_shape)[::-1]
    return jnp.stack([down_half, up_half], axis=1).reshape((LAYERS,) + tail_shape)


def reference(tokens_in, targets, w_in, w_out, norm_gains):
    first_all = to_exec_order(w_in)
    second_all = to_exec_order(w_out)
    gain_all = to_exec_order(norm_gains)
    seed_scale = 2.0 / (MICRO_BATCHES * MICRO_TOKENS)

    def micro_step(loop_state, micro_pair):
        sum_first, sum_second, sum_gain, sse_total = loop_state
        micro_tokens, micro_targets = micro_pair

        def forward_layer(act_in, layer_weights):
            return layer_forward(act_in, layer_weights[0], layer_weights[1], layer_weights[2]), act_in

        final_act, saved_inputs = lax.scan(forward_layer, micro_tokens, (first_all, second_all, gain_all))
        error_f32 = final_act.astype(jnp.float32) - micro_targets.astype(jnp.float32)
        seed_grad = (error_f32 * seed_scale).astype(jnp.bfloat16)

        def backward_layer(grad_h, layer_data):
            grad_x, grad_first, grad_second, grad_gain = layer_backward(
                layer_data[0], grad_h, layer_data[1], layer_data[2], layer_data[3])
            return grad_x, (grad_first, grad_second, grad_gain)

        _, layer_grads = lax.scan(backward_layer, seed_grad,
                                  (saved_inputs, first_all, second_all, gain_all), reverse=True)
        new_state = (sum_first + layer_grads[0], sum_second + layer_grads[1],
                     sum_gain + layer_grads[2], sse_total + jnp.sum(error_f32 * error_f32))
        return new_state, None

    init_state = (jnp.zeros((LAYERS, D_MODEL, D_FF), jnp.float32),
                  jnp.zeros((LAYERS, D_FF, D_MODEL), jnp.float32),
                  jnp.zeros((LAYERS, D_MODEL), jnp.float32),
                  jnp.zeros((), jnp.float32))
    final_state, _ = lax.scan(micro_step, init_state, (tokens_in, targets))
    loss_value = final_state[3] / (MICRO_BATCHES * MICRO_TOKENS * D_MODEL)
    return (to_stored_order(final_state[0]), to_stored_order(final_state[1]),
            to_stored_order(final_state[2]), loss_value.reshape(1))
```

```python
import functools

import jax
import jax.numpy as jnp
from jax import lax
from jax.experimental import pallas as pl
from jax.experimental.pallas import tpu as pltpu
from jax.sharding import PartitionSpec as P

BF = jnp.bfloat16
F32 = jnp.float32
EPSILON = 1e-6
CHUNK = 256
HALVES = 2
NT = (((1,), (1,)), ((), ()))
K0 = 0.7978845608028654
K1 = 0.044715
KIND, MB, GOT, PRE, WA, WB, WC, WW = 1, 4, 64, 128, 256, 512, 1024, 2048
ENTRY = 4096


def make_schedule(stages, chunks, t_fwd, t_bwd, lat_same, lat_chip, lat_far):
    dur = (t_fwd, t_fwd, t_bwd, t_bwd)

    def successor(dev, kind):
        if kind in (0, 2):
            return (dev + 1, kind) if dev < stages - 1 else (dev, kind + 1)
        if dev > 0:
            return (dev - 1, kind)
        return (dev, 2) if kind == 1 else None

    def latency(a, b):
        if a == b:
            return 1.0
        low = min(a, b)
        if low % 2 == 0:
            return lat_same
        return lat_far if low % 4 == 3 else lat_chip

    def tail(dev, kind):
        return {0: 4 * stages - dev, 1: 2 * stages + dev, 2: 2 * stages - dev, 3: dev}[kind]

    def simulate(order_key):
        ready = [dict() for _ in range(stages)]
        for m in range(chunks):
            ready[0][(0, m)] = 0.0
        free = [0.0] * stages
        orders = [[] for _ in range(stages)]
        starts = [[] for _ in range(stages)]
        total = 4 * chunks * stages
        done = 0
        while done < total:
            best = None
            for dev in range(stages):
                if ready[dev]:
                    t = max(free[dev], min(ready[dev].values()))
                    if best is None or t < best[0]:
                        best = (t, dev)
            t, dev = best
            cands = [op for op, r in ready[dev].items() if r <= t + 1e-9]
            op = min(cands, key=lambda o: order_key(dev, o[0], o[1]))
            arrive = ready[dev].pop(op)
            orders[dev].append(op)
            starts[dev].append((t, arrive))
            end = t + dur[op[0]]
            free[dev] = end
            nxt = successor(dev, op[0])
            if nxt is not None:
                ready[nxt[0]][(nxt[1], op[1])] = end + latency(dev, nxt[0])
            done += 1
        return max(free), orders, starts

    keys = [
        lambda d, k, m: (-k, m),
        lambda d, k, m: (m - 0.0 * k, -k),
        lambda d, k, m: (m - 2 * k, -k),
        lambda d, k, m: (m - 4 * k, -k),
        lambda d, k, m: (m - 8 * k, -k),
        lambda d, k, m: (-tail(d, k) + m, k),
        lambda d, k, m: (-tail(d, k) + 4 * m, k),
        lambda d, k, m: (-tail(d, k) + 8 * m, k),
        lambda d, k, m: (k, m),
    ]
    results = [simulate(key) for key in keys]
    return min(results, key=lambda r: r[0])


def encode(stages, chunks, orders, starts, margin):
    rows = []
    for dev in range(stages):
        ops = orders[dev]

        def sends(i):
            return 0 <= i < len(ops) and not (dev == 0 and ops[i][0] == 3)

        def local(i):
            return sends(i) and ((dev == stages - 1 and ops[i][0] in (0, 2)) or (dev == 0 and ops[i][0] == 1))

        def feeds(i):
            return local(i) and i + 1 < len(ops) and ops[i + 1] == (ops[i][0] + 1, ops[i][1])

        row = []
        got = False
        seen_top = False
        for i in range(len(ops) + 1):
            e = 0
            if i < len(ops):
                kind, m = ops[i]
                e += KIND * kind + MB * m
                if got:
                    e += GOT
                got = False
                if i + 1 < len(ops):
                    nk, nm = ops[i + 1]
                    t0 = starts[dev][i][0]
                    arrive = starts[dev][i + 1][1]
                    own = dev == 0 and nk == 0
                    dependent = nm == m and nk == kind + 1
                    came_local = (dev == stages - 1 and nk in (1, 3)) or (dev == 0 and nk == 2)
                    prev_local = came_local and ops[i][1] == nm and ops[i][0] == nk - 1
                    if own or (not dependent and not prev_local and arrive + margin <= t0):
                        e += PRE
                        got = True
                if kind in (1, 2) and not seen_top:
                    e += WW
                    seen_top = True
            if feeds(i - 1):
                e += WA
            elif local(i - 1):
                e += WB
            elif i == len(ops) and sends(i - 1):
                e += WB
            if sends(i - 2) and not local(i - 2):
                e += WC
            row.append(e)
        if len(row) % 2:
            row.append(0)
        rows.append([row[j] + ENTRY * row[j + 1] for j in range(0, len(row), 2)])
    return rows


def gelu_and_slope(a):
    a2 = a * a
    t = jnp.tanh(K0 * (a + K1 * (a * a2)))
    cdf = 0.5 * (1.0 + t)
    return a * cdf, cdf + (0.5 * K0) * a * (1.0 - t * t) * (1.0 + (3.0 * K1) * a2)


def pipeline_kernel(stages, table, seed_scale,
                    tokens, targets, w_in, w_out, gains,
                    xs, dhs, ns, us, gs, das, gain_sum, sse_sum,
                    wi, wo, xin, nx, ub, gt, ob,
                    recv_sem, send_sem, in_sem, w_sem, out_sem, g_sem, x_sem):
    me = lax.axis_index('stage')
    chunks = tokens.shape[0] // CHUNK
    d_model = tokens.shape[1]
    d_ff = w_in.shape[2]
    half = d_ff // HALVES
    first = me == 0
    last = me == stages - 1
    n_ops = 4 * chunks

    def weight_copy(row, which):
        src, dst = ((w_in, wi), (w_out, wo))[which]
        return pltpu.make_async_copy(src.at[row], dst.at[row], w_sem.at[2 * row + which])

    weight_copy(0, 0).start()
    weight_copy(0, 1).start()

    barrier = pltpu.get_barrier_semaphore()

    @pl.when(me > 0)
    def _():
        pl.semaphore_signal(barrier, inc=1, device_id={'stage': jnp.maximum(me - 1, 0)})

    @pl.when(me < stages - 1)
    def _():
        pl.semaphore_signal(barrier, inc=1, device_id={'stage': jnp.minimum(me + 1, stages - 1)})

    @pl.when(first | last)
    def _():
        pl.semaphore_wait(barrier, 1)

    @pl.when(jnp.logical_not(first | last))
    def _():
        pl.semaphore_wait(barrier, 2)

    words = []
    for j in range(len(table[0])):
        word = jnp.int32(table[0][j])
        for dev in range(1, stages):
            word = jnp.where(me == dev, jnp.int32(table[dev][j]), word)
        words.append(word)

    def entry(s):
        word = words[0]
        pair = lax.div(s, 2)
        for j in range(1, len(words)):
            word = jnp.where(pair == j, words[j], word)
        return jnp.where(lax.rem(s, 2) == 0, lax.rem(word, ENTRY), lax.div(word, ENTRY))

    def flag(e, bit):
        return lax.rem(lax.div(e, bit), 2) == 1

    def fields(e):
        kind = lax.rem(e, 4)
        m = lax.rem(lax.div(e, MB), chunks)
        row = jnp.where((kind == 1) | (kind == 2), 1, 0)
        return kind, m, row

    def rows_of(m):
        return pl.ds(pl.multiple_of(m * CHUNK, CHUNK), CHUNK)

    def in_copy(slot):
        return pltpu.make_async_copy(tokens.at[pl.ds(0, CHUNK)], xin.at[slot], in_sem.at[slot])

    def start_input(e, slot):
        kind, m, row = fields(e)
        rows = rows_of(m)
        here = (first & ((kind == 0) | (kind == 2))) | (last & ((kind == 1) | (kind == 3)))

        @pl.when(jnp.logical_not(here))
        def _():
            pltpu.make_async_remote_copy(
                src_ref=ob.at[0], dst_ref=xs.at[row, rows], send_sem=send_sem.at[0],
                recv_sem=recv_sem.at[kind * chunks + m], device_id={'stage': me}).wait_recv()

        @pl.when((kind == 0) & first)
        def _():
            pltpu.make_async_copy(tokens.at[rows], xin.at[slot], in_sem.at[slot]).start()

        @pl.when((kind < 2) & jnp.logical_not((kind == 0) & first))
        def _():
            pltpu.make_async_copy(xs.at[row, rows], xin.at[slot], in_sem.at[slot]).start()

        @pl.when(kind >= 2)
        def _():
            pltpu.make_async_copy(dhs.at[row, rows], xin.at[slot], in_sem.at[slot]).start()

    def sent(slot):
        return pltpu.make_async_copy(ob.at[slot], xs.at[0, pl.ds(0, CHUNK)], send_sem.at[slot])

    def slope_copy_in(row, rows, h):
        return pltpu.make_async_copy(gs.at[row, rows, pl.ds(h * half, half)], gt.at[h], g_sem.at[h])

    def start_slopes(e, halves):
        kind, m, row = fields(e)

        @pl.when(kind >= 2)
        def _():
            for h in halves:
                slope_copy_in(row, rows_of(m), h).start()

    def mid_step(s, e, e_next, slot):
        @pl.when(flag(e, WB))
        def _():
            sent(1 - slot).wait()

        @pl.when(flag(e, WC))
        def _():
            sent(slot).wait()

        @pl.when(flag(e, PRE))
        def _():
            start_input(e_next, 1 - slot)

    gain_sum[...] = jnp.zeros_like(gain_sum)
    sse_sum[...] = jnp.zeros_like(sse_sum)
    weight_copy(0, 0).wait()
    weight_copy(0, 1).wait()
    weight_copy(1, 0).start()
    weight_copy(1, 1).start()

    BLK = 64

    def step(s, carry):
        e = entry(s)
        e_next = jnp.where(s + 1 < n_ops, entry(s + 1), 0)
        kind, m, row = fields(e)
        rows = rows_of(m)
        slot = lax.rem(s, 2)

        @pl.when(flag(e, WA))
        def _():
            sent(1 - slot).wait()

        @pl.when(jnp.logical_not(flag(e, GOT)))
        def _():
            start_input(e, slot)

        @pl.when(flag(e, WW))
        def _():
            weight_copy(1, 0).wait()
            weight_copy(1, 1).wait()

        @pl.when(kind < 2)
        def _():
            in_copy(slot).wait()
            gain = gains[row]

            @pl.loop(0, CHUNK // BLK)
            def _(b):
                rb = pl.ds(pl.multiple_of(b * BLK, BLK), BLK)
                x = xin[slot, rb].astype(F32)
                inv = lax.rsqrt(jnp.mean(x * x, axis=-1, keepdims=True) + EPSILON)
                nx[rb] = (x * inv * gain).astype(BF)

            n_copy = pltpu.make_async_copy(nx, ns.at[row, rows], out_sem.at[0])
            n_copy.start()
            g_copies = []
            for h in range(HALVES):
                for j in range(half // 512):
                    lo = h * half + j * 512
                    a = jnp.dot(nx[...], wi[row, :, lo:lo + 512], preferred_element_type=F32)
                    for b in range(CHUNK // 16):
                        u, g = gelu_and_slope(a[b * 16:(b + 1) * 16])
                        ub[b * 16:(b + 1) * 16, lo:lo + 512] = u.astype(BF)
                        gt[h, b * 16:(b + 1) * 16, j * 512:(j + 1) * 512] = g
                g_copy = pltpu.make_async_copy(gt.at[h], gs.at[row, rows, pl.ds(h * half, half)], g_sem.at[h])
                g_copy.start()
                g_copies.append(g_copy)
            u_copy = pltpu.make_async_copy(ub, us.at[row, rows], out_sem.at[1])
            u_copy.start()
            mid_step(s, e, e_next, slot)
            for j in range(d_model // 256):
                cols = slice(j * 256, (j + 1) * 256)
                y = jnp.dot(ub[...], wo[row, :, cols], preferred_element_type=F32)
                ob[slot, :, cols] = (xin[slot, :, cols].astype(F32) + y).astype(BF)
            n_copy.wait()

            @pl.when(first & (kind == 1))
            def _():
                seed_copy = pltpu.make_async_copy(targets.at[rows], nx, x_sem)
                seed_copy.start()
                seed_copy.wait()

                @pl.loop(0, CHUNK // BLK)
                def _(b):
                    rb = pl.ds(pl.multiple_of(b * BLK, BLK), BLK)
                    err = ob[slot, rb].astype(F32) - nx[rb].astype(F32)
                    ob[slot, rb] = (err * seed_scale).astype(BF)
                    sse_sum[...] += jnp.sum((err * err).reshape(BLK // 8, 8, d_model), axis=0)

            u_copy.wait()
            for g_copy in g_copies:
                g_copy.wait()
            send(kind, m, row, rows, slot)
            start_slopes(e_next, (0, 1))

        @pl.when(kind >= 2)
        def _():
            @pl.when((kind == 3) & first)
            def _():
                pltpu.make_async_copy(tokens.at[rows], nx, x_sem).start()

            @pl.when(jnp.logical_not((kind == 3) & first))
            def _():
                pltpu.make_async_copy(xs.at[row, rows], nx, x_sem).start()

            in_copy(slot).wait()
            for h in range(HALVES):
                slope_copy_in(row, rows, h).wait()
                for j in range(half // 512):
                    lo = h * half + j * 512
                    du = lax.dot_general(xin[slot], wo[row, lo:lo + 512, :], NT, preferred_element_type=F32)
                    ub[:, lo:lo + 512] = (du * gt[h, :, j * 512:(j + 1) * 512]).astype(BF)
            da_copy = pltpu.make_async_copy(ub, das.at[row, rows], out_sem.at[1])
            da_copy.start()
            start_slopes(e_next, (0,))
            mid_step(s, e, e_next, slot)
            for j in range(d_model // 256):
                cols = slice(j * 256, (j + 1) * 256)
                gt[1, :, cols] = lax.dot_general(ub[...], wi[row, cols, :], NT, preferred_element_type=F32)
            pltpu.make_async_copy(tokens.at[pl.ds(0, CHUNK)], nx, x_sem).wait()
            gain = gains[row]

            @pl.loop(0, CHUNK // BLK)
            def _(b):
                rb = pl.ds(pl.multiple_of(b * BLK, BLK), BLK)
                x = nx[rb].astype(F32)
                inv = lax.rsqrt(jnp.mean(x * x, axis=-1, keepdims=True) + EPSILON)
                grad_n = gt[1, rb, :d_model]
                q = grad_n * gain
                proj = jnp.mean(q * x, axis=-1, keepdims=True)
                dx = q * inv - x * (inv * inv * inv * proj)
                ob[slot, rb] = (xin[slot, rb].astype(F32) + dx).astype(BF)
                gain_sum[row] += jnp.sum((grad_n * x * inv).reshape(BLK // 8, 8, d_model), axis=0)

            start_slopes(e_next, (1,))
            da_copy.wait()
            send(kind, m, row, rows, slot)

        return carry

    def send(kind, m, row, rows, slot):
        down = (kind == 0) | (kind == 2)
        turn = (last & down) | (first & (kind == 1))
        stop = first & (kind == 3)
        to = jnp.where(down, jnp.minimum(me + 1, stages - 1), jnp.maximum(me - 1, 0))
        remote = jnp.logical_not(turn | stop)

        @pl.when(remote & (kind < 2))
        def _():
            pltpu.make_async_remote_copy(
                src_ref=ob.at[slot], dst_ref=xs.at[row, rows], send_sem=send_sem.at[slot],
                recv_sem=recv_sem.at[kind * chunks + m], device_id={'stage': to}).start()

        @pl.when(remote & (kind >= 2))
        def _():
            pltpu.make_async_remote_copy(
                src_ref=ob.at[slot], dst_ref=dhs.at[row, rows], send_sem=send_sem.at[slot],
                recv_sem=recv_sem.at[kind * chunks + m], device_id={'stage': to}).start()

        @pl.when(turn & (kind == 0))
        def _():
            pltpu.make_async_copy(ob.at[slot], xs.at[1, rows], send_sem.at[slot]).start()

        @pl.when(turn & (kind == 1))
        def _():
            pltpu.make_async_copy(ob.at[slot], dhs.at[1, rows], send_sem.at[slot]).start()

        @pl.when(turn & (kind == 2))
        def _():
            pltpu.make_async_copy(ob.at[slot], dhs.at[0, rows], send_sem.at[slot]).start()

    lax.fori_loop(0, n_ops, step, 0)
    e_end = entry(jnp.int32(n_ops))

    @pl.when(flag(e_end, WB))
    def _():
        sent((n_ops - 1) % 2).wait()

    @pl.when(flag(e_end, WC))
    def _():
        sent(n_ops % 2).wait()


def solution(mesh):
    stages = mesh.shape['stage']

    def device_step(tokens, targets, w_in, w_out, norm_gains):
        micro_count, tokens_mb, d_model = tokens.shape
        d_ff = w_in.shape[2]
        total = micro_count * tokens_mb
        chunks = total // CHUNK
        _, orders, starts = make_schedule(stages, chunks, 8.3, 8.0, 2.5, 9.5, 10.5)
        table = encode(stages, chunks, orders, starts, 2.0)
        any_spec = pl.BlockSpec(memory_space=pl.ANY)
        vmem_spec = pl.BlockSpec(memory_space=pltpu.VMEM)
        shape = jax.ShapeDtypeStruct
        xs, dhs, ns, us, gs, das, gain_sum, sse_sum = pl.pallas_call(
            functools.partial(pipeline_kernel, stages, table, 2.0 / total),
            out_shape=[shape((2, total, d_model), BF), shape((2, total, d_model), BF),
                       shape((2, total, d_model), BF), shape((2, total, d_ff), BF),
                       shape((2, total, d_ff), F32), shape((2, total, d_ff), BF),
                       shape((2, 8, d_model), F32), shape((8, d_model), F32)],
            in_specs=[any_spec] * 4 + [vmem_spec],
            out_specs=[any_spec] * 6 + [vmem_spec] * 2,
            scratch_shapes=[
                pltpu.VMEM((2, d_model, d_ff), BF), pltpu.VMEM((2, d_ff, d_model), BF),
                pltpu.VMEM((2, CHUNK, d_model), BF), pltpu.VMEM((CHUNK, d_model), BF),
                pltpu.VMEM((CHUNK, d_ff), BF), pltpu.VMEM((HALVES, CHUNK, d_ff // HALVES), F32),
                pltpu.VMEM((2, CHUNK, d_model), BF),
                pltpu.SemaphoreType.DMA((4 * chunks,)), pltpu.SemaphoreType.DMA((2,)),
                pltpu.SemaphoreType.DMA((2,)), pltpu.SemaphoreType.DMA((4,)),
                pltpu.SemaphoreType.DMA((2,)), pltpu.SemaphoreType.DMA((HALVES,)),
                pltpu.SemaphoreType.DMA,
            ],
            compiler_params=pltpu.CompilerParams(
                collective_id=0, has_side_effects=True, vmem_limit_bytes=67043328),
            name='vee',
        )(tokens.reshape(total, d_model), targets.reshape(total, d_model), w_in, w_out,
          norm_gains.reshape(2, 1, d_model))
        del xs, gs
        tok = (((1,), (1,)), ((0,), (0,)))
        grad_w_in = lax.dot_general(ns, das, tok, preferred_element_type=F32)
        grad_w_out = lax.dot_general(us, dhs, tok, preferred_element_type=F32)
        grad_gains = jnp.sum(gain_sum, axis=1)
        sse = jnp.where(lax.axis_index('stage') == 0, jnp.sum(sse_sum), 0.0)
        loss_value = lax.psum(sse, 'stage') / (total * d_model)
        return grad_w_in, grad_w_out, grad_gains, loss_value.reshape(1)

    block_spec = P(('dp', 'stage'))
    return jax.shard_map(device_step, mesh=mesh,
                         in_specs=(P('dp'), P('dp'), P('stage'), P('stage'), P('stage')),
                         out_specs=(block_spec, block_spec, block_spec, P('dp')),
                         check_vma=False)
```

```python
import functools

import jax
import jax.numpy as jnp
from jax import lax
from jax.experimental import pallas as pl
from jax.experimental.pallas import tpu as pltpu
from jax.sharding import PartitionSpec as P

BF = jnp.bfloat16
F32 = jnp.float32
EPSILON = 1e-6
CHUNK = 256
HALVES = 2
NT = (((1,), (1,)), ((), ()))
K0 = 0.7978845608028654
K1 = 0.044715
KIND, MB, GOT, PRE, WA, WB, WC, WW = 1, 4, 64, 128, 256, 512, 1024, 2048
ENTRY = 4096


def make_schedule(stages, chunks, t_fwd, t_bwd, lat_same, lat_chip, lat_far):
    dur = (t_fwd, t_fwd, t_bwd, t_bwd)

    def successor(dev, kind):
        if kind in (0, 2):
            return (dev + 1, kind) if dev < stages - 1 else (dev, kind + 1)
        if dev > 0:
            return (dev - 1, kind)
        return (dev, 2) if kind == 1 else None

    def latency(a, b):
        if a == b:
            return 2.5
        low = min(a, b)
        if low % 2 == 0:
            return lat_same
        return lat_far if low % 4 == 3 else lat_chip

    def tail(dev, kind):
        return {0: 4 * stages - dev, 1: 2 * stages + dev, 2: 2 * stages - dev, 3: dev}[kind]

    def simulate(order_key):
        ready = [dict() for _ in range(stages)]
        for m in range(chunks):
            ready[0][(0, m)] = 0.0
        free = [0.0] * stages
        orders = [[] for _ in range(stages)]
        starts = [[] for _ in range(stages)]
        total = 4 * chunks * stages
        done = 0
        while done < total:
            best = None
            for dev in range(stages):
                if ready[dev]:
                    t = max(free[dev], min(ready[dev].values()))
                    if best is None or t < best[0]:
                        best = (t, dev)
            t, dev = best
            cands = [op for op, r in ready[dev].items() if r <= t + 1e-9]
            op = min(cands, key=lambda o: order_key(dev, o[0], o[1]))
            arrive = ready[dev].pop(op)
            orders[dev].append(op)
            starts[dev].append((t, arrive))
            end = t + dur[op[0]]
            free[dev] = end
            nxt = successor(dev, op[0])
            if nxt is not None:
                ready[nxt[0]][(nxt[1], op[1])] = end + latency(dev, nxt[0])
            done += 1
        return max(free), orders, starts

    keys = [
        lambda d, k, m: (-k, m),
        lambda d, k, m: (m - 0.0 * k, -k),
        lambda d, k, m: (m - 2 * k, -k),
        lambda d, k, m: (m - 4 * k, -k),
        lambda d, k, m: (m - 8 * k, -k),
        lambda d, k, m: (-tail(d, k) + m, k),
        lambda d, k, m: (-tail(d, k) + 4 * m, k),
        lambda d, k, m: (-tail(d, k) + 8 * m, k),
        lambda d, k, m: (k, m),
    ]
    results = [simulate(key) for key in keys]
    return min(results, key=lambda r: r[0])


def encode(stages, chunks, orders, starts, margin):
    rows = []
    for dev in range(stages):
        ops = orders[dev]

        def sends(i):
            return 0 <= i < len(ops) and not (dev == 0 and ops[i][0] == 3)

        def local(i):
            return sends(i) and ((dev == stages - 1 and ops[i][0] in (0, 2)) or (dev == 0 and ops[i][0] == 1))

        def feeds(i):
            return local(i) and i + 1 < len(ops) and ops[i + 1] == (ops[i][0] + 1, ops[i][1])

        row = []
        got = False
        seen_top = False
        for i in range(len(ops) + 1):
            e = 0
            if i < len(ops):
                kind, m = ops[i]
                e += KIND * kind + MB * m
                if got:
                    e += GOT
                got = False
                if i + 1 < len(ops):
                    nk, nm = ops[i + 1]
                    t0 = starts[dev][i][0]
                    arrive = starts[dev][i + 1][1]
                    own = dev == 0 and nk == 0
                    dependent = nm == m and nk == kind + 1
                    came_local = (dev == stages - 1 and nk in (1, 3)) or (dev == 0 and nk == 2)
                    prev_local = came_local and ops[i][1] == nm and ops[i][0] == nk - 1
                    if own or (not dependent and not prev_local and arrive + margin <= t0):
                        e += PRE
                        got = True
                if kind in (1, 2) and not seen_top:
                    e += WW
                    seen_top = True
            if feeds(i - 1):
                e += WA
            elif local(i - 1):
                e += WB
            elif i == len(ops) and sends(i - 1):
                e += WB
            if sends(i - 2) and not local(i - 2):
                e += WC
            row.append(e)
        if len(row) % 2:
            row.append(0)
        rows.append([row[j] + ENTRY * row[j + 1] for j in range(0, len(row), 2)])
    return rows


def gelu_and_slope(a):
    a2 = a * a
    cdf = 0.5 * jnp.tanh(a * (K0 + (K0 * K1) * a2)) + 0.5
    u = a * cdf
    return u, cdf + (u * (1.0 - cdf)) * (2.0 * K0 + (6.0 * K0 * K1) * a2)


def pipeline_kernel(stages, table, seed_scale,
                    tokens, targets, w_in, w_out, gains,
                    xs, dhs, ns, us, gs, das, gain_sum, sse_sum,
                    wi, wo, xin, nx, ub, gt, ob, sse_acc, sse_in,
                    recv_sem, send_sem, in_sem, w_sem, out_sem, g_sem, x_sem, sse_send, sse_recv):
    me = lax.axis_index('stage')
    chunks = tokens.shape[0] // CHUNK
    d_model = tokens.shape[1]
    d_ff = w_in.shape[2]
    half = d_ff // HALVES
    first = me == 0
    last = me == stages - 1
    n_ops = 4 * chunks

    def weight_copies(row):
        copies = [pltpu.make_async_copy(w_in.at[row, :, pl.ds(h * half, half)], wi.at[row, h],
                                        w_sem.at[3 * row + h]) for h in range(HALVES)]
        return copies + [pltpu.make_async_copy(w_out.at[row], wo.at[row], w_sem.at[3 * row + HALVES])]

    for copy in weight_copies(0):
        copy.start()

    barrier = pltpu.get_barrier_semaphore()

    @pl.when(me > 0)
    def _():
        pl.semaphore_signal(barrier, inc=1, device_id={'stage': jnp.maximum(me - 1, 0)})

    @pl.when(me < stages - 1)
    def _():
        pl.semaphore_signal(barrier, inc=1, device_id={'stage': jnp.minimum(me + 1, stages - 1)})

    @pl.when(me > 1)
    def _():
        pl.semaphore_signal(barrier, inc=1, device_id={'stage': 0})

    @pl.when(first)
    def _():
        pl.semaphore_wait(barrier, stages - 1)

    @pl.when(last)
    def _():
        pl.semaphore_wait(barrier, 1)

    @pl.when(jnp.logical_not(first | last))
    def _():
        pl.semaphore_wait(barrier, 2)

    words = []
    for j in range(len(table[0])):
        word = jnp.int32(table[0][j])
        for dev in range(1, stages):
            word = jnp.where(me == dev, jnp.int32(table[dev][j]), word)
        words.append(word)

    def entry(s):
        word = words[0]
        pair = lax.div(s, 2)
        for j in range(1, len(words)):
            word = jnp.where(pair == j, words[j], word)
        return jnp.where(lax.rem(s, 2) == 0, lax.rem(word, ENTRY), lax.div(word, ENTRY))

    def flag(e, bit):
        return lax.rem(lax.div(e, bit), 2) == 1

    def fields(e):
        kind = lax.rem(e, 4)
        m = lax.rem(lax.div(e, MB), chunks)
        row = jnp.where((kind == 1) | (kind == 2), 1, 0)
        return kind, m, row

    def rows_of(m):
        return pl.ds(pl.multiple_of(m * CHUNK, CHUNK), CHUNK)

    def in_copy(slot):
        return pltpu.make_async_copy(tokens.at[pl.ds(0, CHUNK)], xin.at[slot], in_sem.at[slot])

    def start_input(e, slot):
        kind, m, row = fields(e)
        rows = rows_of(m)
        here = (first & ((kind == 0) | (kind == 2))) | (last & ((kind == 1) | (kind == 3)))

        @pl.when(jnp.logical_not(here))
        def _():
            pltpu.make_async_remote_copy(
                src_ref=ob.at[0], dst_ref=xs.at[row, rows], send_sem=send_sem.at[0],
                recv_sem=recv_sem.at[kind * chunks + m], device_id={'stage': me}).wait_recv()

        @pl.when((kind == 0) & first)
        def _():
            pltpu.make_async_copy(tokens.at[rows], xin.at[slot], in_sem.at[slot]).start()

        @pl.when((kind < 2) & jnp.logical_not((kind == 0) & first))
        def _():
            pltpu.make_async_copy(xs.at[row, rows], xin.at[slot], in_sem.at[slot]).start()

        @pl.when(kind >= 2)
        def _():
            pltpu.make_async_copy(dhs.at[row, rows], xin.at[slot], in_sem.at[slot]).start()

    def sent(slot):
        return pltpu.make_async_copy(ob.at[slot], xs.at[0, pl.ds(0, CHUNK)], send_sem.at[slot])

    def slope_copy_in(row, rows, h):
        return pltpu.make_async_copy(gs.at[row, rows, pl.ds(h * half, half)], gt.at[h], g_sem.at[h])

    def start_slopes(e, halves):
        kind, m, row = fields(e)

        @pl.when(kind >= 2)
        def _():
            for h in halves:
                slope_copy_in(row, rows_of(m), h).start()

    def mid_step(s, e, e_next, slot):
        @pl.when(flag(e, WB))
        def _():
            sent(1 - slot).wait()

        @pl.when(flag(e, WC))
        def _():
            sent(slot).wait()

        @pl.when(flag(e, PRE))
        def _():
            start_input(e_next, 1 - slot)

    gain_sum[...] = jnp.zeros_like(gain_sum)
    sse_acc[...] = jnp.zeros_like(sse_acc)
    for copy in weight_copies(0):
        copy.wait()
    for copy in weight_copies(1):
        copy.start()

    def sse_copy(dev):
        return pltpu.make_async_remote_copy(
            src_ref=sse_sum, dst_ref=sse_in, send_sem=sse_send.at[dev], recv_sem=sse_recv,
            device_id={'stage': dev})

    BLK = 64

    def step(s, carry):
        e = entry(s)
        e_next = jnp.where(s + 1 < n_ops, entry(s + 1), 0)
        kind, m, row = fields(e)
        rows = rows_of(m)
        slot = lax.rem(s, 2)

        @pl.when(flag(e, WA))
        def _():
            sent(1 - slot).wait()

        @pl.when(jnp.logical_not(flag(e, GOT)))
        def _():
            start_input(e, slot)

        @pl.when(flag(e, WW))
        def _():
            for copy in weight_copies(1):
                copy.wait()

        @pl.when(kind < 2)
        def _():
            in_copy(slot).wait()
            gain = gains[row]

            @pl.loop(0, CHUNK // BLK)
            def _(b):
                rb = pl.ds(pl.multiple_of(b * BLK, BLK), BLK)
                x = xin[slot, rb].astype(F32)
                inv = lax.rsqrt(jnp.mean(x * x, axis=-1, keepdims=True) + EPSILON)
                nx[rb] = (x * inv * gain).astype(BF)

            n_copy = pltpu.make_async_copy(nx, ns.at[row, rows], out_sem.at[0])
            n_copy.start()
            g_copies = []
            u_copies = []
            for h in range(HALVES):
                for j in range(half // 512):
                    a = jnp.dot(nx[...], wi[row, h, :, j * 512:(j + 1) * 512], preferred_element_type=F32)
                    for b in range(CHUNK // 16):
                        u, g = gelu_and_slope(a[b * 16:(b + 1) * 16])
                        ub[h, b * 16:(b + 1) * 16, j * 512:(j + 1) * 512] = u.astype(BF)
                        gt[h, b * 16:(b + 1) * 16, j * 512:(j + 1) * 512] = g
                g_copy = pltpu.make_async_copy(gt.at[h], gs.at[row, rows, pl.ds(h * half, half)], g_sem.at[h])
                g_copy.start()
                g_copies.append(g_copy)
                u_copy = pltpu.make_async_copy(ub.at[h], us.at[row, rows, pl.ds(h * half, half)],
                                               out_sem.at[1 + h])
                u_copy.start()
                u_copies.append(u_copy)
            mid_step(s, e, e_next, slot)

            def second(rb, cols):
                y = jnp.dot(ub[0, rb, :], wo[row, :half, cols], preferred_element_type=F32)
                y += jnp.dot(ub[1, rb, :], wo[row, half:, cols], preferred_element_type=F32)
                ob[slot, rb, cols] = (xin[slot, rb, cols].astype(F32) + y).astype(BF)

            for j in range(d_model // 256 - 1):
                second(slice(0, CHUNK), slice(j * 256, (j + 1) * 256))
            for g_copy in g_copies:
                g_copy.wait()
            start_slopes(e_next, (0, 1))
            second(slice(0, CHUNK // 2), slice(d_model - 256, d_model))
            second(slice(CHUNK // 2, CHUNK), slice(d_model - 256, d_model))
            n_copy.wait()

            @pl.when(first & (kind == 1))
            def _():
                seed_copy = pltpu.make_async_copy(targets.at[rows], nx, x_sem)
                seed_copy.start()
                seed_copy.wait()

                @pl.loop(0, CHUNK // BLK)
                def _(b):
                    rb = pl.ds(pl.multiple_of(b * BLK, BLK), BLK)
                    err = ob[slot, rb].astype(F32) - nx[rb].astype(F32)
                    ob[slot, rb] = (err * seed_scale).astype(BF)
                    sse_acc[...] += jnp.sum((err * err).reshape(BLK // 8, 8, d_model), axis=0)

                @pl.when(m == chunks - 1)
                def _():
                    acc = sse_acc[:, :128]
                    for j in range(1, d_model // 128):
                        acc += sse_acc[:, j * 128:(j + 1) * 128]
                    sse_sum[...] = acc

            for u_copy in u_copies:
                u_copy.wait()
            send(kind, m, row, rows, slot)

            @pl.when(first & (kind == 1) & (m == chunks - 1))
            def _():
                for dev in range(1, stages):
                    sse_copy(dev).start()

        @pl.when(kind >= 2)
        def _():
            @pl.when((kind == 3) & first)
            def _():
                pltpu.make_async_copy(tokens.at[rows], nx, x_sem).start()

            @pl.when(jnp.logical_not((kind == 3) & first))
            def _():
                pltpu.make_async_copy(xs.at[row, rows], nx, x_sem).start()

            in_copy(slot).wait()
            for h in range(HALVES):
                slope_copy_in(row, rows, h).wait()
                for j in range(half // 512):
                    lo = h * half + j * 512
                    du = lax.dot_general(xin[slot], wo[row, lo:lo + 512, :], NT, preferred_element_type=F32)
                    ub[h, :, j * 512:(j + 1) * 512] = (du * gt[h, :, j * 512:(j + 1) * 512]).astype(BF)
            da_copies = [pltpu.make_async_copy(ub.at[h], das.at[row, rows, pl.ds(h * half, half)],
                                               out_sem.at[1 + h]) for h in range(HALVES)]
            for da_copy in da_copies:
                da_copy.start()
            start_slopes(e_next, (0,))
            mid_step(s, e, e_next, slot)
            for j in range(d_model // 256 - 1):
                cols = slice(j * 256, (j + 1) * 256)
                gt[1, :, cols] = (
                    lax.dot_general(ub[0], wi[row, 0, cols, :], NT, preferred_element_type=F32)
                    + lax.dot_general(ub[1], wi[row, 1, cols, :], NT, preferred_element_type=F32))
            for h in range(HALVES):
                gt[1, :, d_model + (h - 1) * 256:d_model + h * 256] = lax.dot_general(
                    ub[h], wi[row, h, d_model - 256:, :], NT, preferred_element_type=F32)
            gt[1, :, d_model - 256:d_model] += gt[1, :, d_model:d_model + 256]
            pltpu.make_async_copy(tokens.at[pl.ds(0, CHUNK)], nx, x_sem).wait()
            gain = gains[row]

            @pl.loop(0, CHUNK // BLK)
            def _(b):
                rb = pl.ds(pl.multiple_of(b * BLK, BLK), BLK)
                x = nx[rb].astype(F32)
                inv = lax.rsqrt(jnp.mean(x * x, axis=-1, keepdims=True) + EPSILON)
                grad_n = gt[1, rb, :d_model]
                q = grad_n * gain
                proj = jnp.mean(q * x, axis=-1, keepdims=True)
                dx = q * inv - x * (inv * inv * inv * proj)
                ob[slot, rb] = (xin[slot, rb].astype(F32) + dx).astype(BF)
                gain_sum[row] += jnp.sum((grad_n * x * inv).reshape(BLK // 8, 8, d_model), axis=0)

            start_slopes(e_next, (1,))
            for da_copy in da_copies:
                da_copy.wait()
            send(kind, m, row, rows, slot)

        return carry

    def send(kind, m, row, rows, slot):
        down = (kind == 0) | (kind == 2)
        turn = (last & down) | (first & (kind == 1))
        stop = first & (kind == 3)
        to = jnp.where(down, jnp.minimum(me + 1, stages - 1), jnp.maximum(me - 1, 0))
        remote = jnp.logical_not(turn | stop)

        @pl.when(remote & (kind < 2))
        def _():
            pltpu.make_async_remote_copy(
                src_ref=ob.at[slot], dst_ref=xs.at[row, rows], send_sem=send_sem.at[slot],
                recv_sem=recv_sem.at[kind * chunks + m], device_id={'stage': to}).start()

        @pl.when(remote & (kind >= 2))
        def _():
            pltpu.make_async_remote_copy(
                src_ref=ob.at[slot], dst_ref=dhs.at[row, rows], send_sem=send_sem.at[slot],
                recv_sem=recv_sem.at[kind * chunks + m], device_id={'stage': to}).start()

        @pl.when(turn & (kind == 0))
        def _():
            pltpu.make_async_copy(ob.at[slot], xs.at[1, rows], send_sem.at[slot]).start()

        @pl.when(turn & (kind == 1))
        def _():
            pltpu.make_async_copy(ob.at[slot], dhs.at[1, rows], send_sem.at[slot]).start()

        @pl.when(turn & (kind == 2))
        def _():
            pltpu.make_async_copy(ob.at[slot], dhs.at[0, rows], send_sem.at[slot]).start()

    lax.fori_loop(0, n_ops, step, 0)
    e_end = entry(jnp.int32(n_ops))

    @pl.when(flag(e_end, WB))
    def _():
        sent((n_ops - 1) % 2).wait()

    @pl.when(flag(e_end, WC))
    def _():
        sent(n_ops % 2).wait()

    @pl.when(first)
    def _():
        for dev in range(1, stages):
            sse_copy(dev).wait_send()

    @pl.when(jnp.logical_not(first))
    def _():
        sse_copy(0).wait_recv()
        sse_sum[...] = sse_in[...]


def solution(mesh):
    stages = mesh.shape['stage']

    def device_step(tokens, targets, w_in, w_out, norm_gains):
        micro_count, tokens_mb, d_model = tokens.shape
        d_ff = w_in.shape[2]
        total = micro_count * tokens_mb
        chunks = total // CHUNK
        _, orders, starts = make_schedule(stages, chunks, 10.5, 9.5, 2.7, 9.5, 10.5)
        table = encode(stages, chunks, orders, starts, 2.0)
        any_spec = pl.BlockSpec(memory_space=pl.ANY)
        vmem_spec = pl.BlockSpec(memory_space=pltpu.VMEM)
        shape = jax.ShapeDtypeStruct
        xs, dhs, ns, us, gs, das, gain_sum, sse_sum = pl.pallas_call(
            functools.partial(pipeline_kernel, stages, table, 2.0 / total),
            out_shape=[shape((2, total, d_model), BF), shape((2, total, d_model), BF),
                       shape((2, total, d_model), BF), shape((2, total, d_ff), BF),
                       shape((2, total, d_ff), F32), shape((2, total, d_ff), BF),
                       shape((2, 8, d_model), F32), shape((8, 128), F32)],
            in_specs=[any_spec] * 4 + [vmem_spec],
            out_specs=[any_spec] * 6 + [vmem_spec] * 2,
            scratch_shapes=[
                pltpu.VMEM((2, HALVES, d_model, d_ff // HALVES), BF), pltpu.VMEM((2, d_ff, d_model), BF),
                pltpu.VMEM((2, CHUNK, d_model), BF), pltpu.VMEM((CHUNK, d_model), BF),
                pltpu.VMEM((HALVES, CHUNK, d_ff // HALVES), BF), pltpu.VMEM((HALVES, CHUNK, d_ff // HALVES), F32),
                pltpu.VMEM((2, CHUNK, d_model), BF), pltpu.VMEM((8, d_model), F32),
                pltpu.VMEM((8, 128), F32),
                pltpu.SemaphoreType.DMA((4 * chunks,)), pltpu.SemaphoreType.DMA((2,)),
                pltpu.SemaphoreType.DMA((2,)), pltpu.SemaphoreType.DMA((2 * HALVES + 2,)),
                pltpu.SemaphoreType.DMA((HALVES + 1,)), pltpu.SemaphoreType.DMA((HALVES,)),
                pltpu.SemaphoreType.DMA, pltpu.SemaphoreType.DMA((stages,)), pltpu.SemaphoreType.DMA,
            ],
            compiler_params=pltpu.CompilerParams(
                collective_id=0, has_side_effects=True, vmem_limit_bytes=67043328),
            name='vee',
        )(tokens.reshape(total, d_model), targets.reshape(total, d_model), w_in, w_out,
          norm_gains.reshape(2, 1, d_model))
        del xs, gs
        tok = (((1,), (1,)), ((0,), (0,)))
        grad_w_in = lax.dot_general(ns, das, tok, preferred_element_type=F32)
        grad_w_out = lax.dot_general(us, dhs, tok, preferred_element_type=F32)
        grad_gains = jnp.sum(gain_sum, axis=1)
        loss_value = jnp.sum(sse_sum) / (total * d_model)
        return grad_w_in, grad_w_out, grad_gains, loss_value.reshape(1)

    block_spec = P(('dp', 'stage'))
    return jax.shard_map(device_step, mesh=mesh,
                         in_specs=(P('dp'), P('dp'), P('stage'), P('stage'), P('stage')),
                         out_specs=(block_spec, block_spec, block_spec, P('dp')),
                         check_vma=False)
```

```python
import functools

import jax
import jax.numpy as jnp
from jax import lax
from jax.experimental import pallas as pl
from jax.experimental.pallas import tpu as pltpu
from jax.sharding import PartitionSpec as P

BF = jnp.bfloat16
F32 = jnp.float32
EPSILON = 1e-6
CHUNK = 256
SUB = 128
HALVES = 2
NT = (((1,), (1,)), ((), ()))
K0 = 0.7978845608028654
K1 = 0.044715
KIND, MB, GOT, PRE, WA, WB, WC, WW = 1, 4, 64, 128, 256, 512, 1024, 2048
ENTRY = 4096


def make_schedule(stages, chunks, t_fwd, t_bwd, lat_same, lat_chip, lat_far):
    dur = (t_fwd, t_fwd, t_bwd, t_bwd)

    def successor(dev, kind):
        if kind in (0, 2):
            return (dev + 1, kind) if dev < stages - 1 else (dev, kind + 1)
        if dev > 0:
            return (dev - 1, kind)
        return (dev, 2) if kind == 1 else None

    def latency(a, b):
        if a == b:
            return 2.5
        low = min(a, b)
        if low % 2 == 0:
            return lat_same
        return lat_far if low % 4 == 3 else lat_chip

    def tail(dev, kind):
        return {0: 4 * stages - dev, 1: 2 * stages + dev, 2: 2 * stages - dev, 3: dev}[kind]

    def simulate(order_key):
        ready = [dict() for _ in range(stages)]
        for m in range(chunks):
            ready[0][(0, m)] = 0.0
        free = [0.0] * stages
        orders = [[] for _ in range(stages)]
        starts = [[] for _ in range(stages)]
        total = 4 * chunks * stages
        done = 0
        while done < total:
            best = None
            for dev in range(stages):
                if ready[dev]:
                    t = max(free[dev], min(ready[dev].values()))
                    if best is None or t < best[0]:
                        best = (t, dev)
            t, dev = best
            cands = [op for op, r in ready[dev].items() if r <= t + 1e-9]
            op = min(cands, key=lambda o: order_key(dev, o[0], o[1]))
            arrive = ready[dev].pop(op)
            orders[dev].append(op)
            starts[dev].append((t, arrive))
            end = t + dur[op[0]]
            free[dev] = end
            nxt = successor(dev, op[0])
            if nxt is not None:
                wait = latency(dev, nxt[0])
                if op[0] < 2 and dev != nxt[0]:
                    wait = 0.5 * (wait + 1.5) - 0.5 * t_fwd
                ready[nxt[0]][(nxt[1], op[1])] = end + wait
            done += 1
        return max(free), orders, starts

    keys = [
        lambda d, k, m: (-k, m),
        lambda d, k, m: (m - 0.0 * k, -k),
        lambda d, k, m: (m - 2 * k, -k),
        lambda d, k, m: (m - 4 * k, -k),
        lambda d, k, m: (m - 8 * k, -k),
        lambda d, k, m: (-tail(d, k) + m, k),
        lambda d, k, m: (-tail(d, k) + 4 * m, k),
        lambda d, k, m: (-tail(d, k) + 8 * m, k),
        lambda d, k, m: (k, m),
    ]
    results = [simulate(key) for key in keys]
    return min(results, key=lambda r: r[0])


def encode(stages, chunks, orders, starts, margin):
    rows = []
    for dev in range(stages):
        ops = orders[dev]

        def sends(i):
            return 0 <= i < len(ops) and not (dev == 0 and ops[i][0] == 3)

        def local(i):
            return sends(i) and ((dev == stages - 1 and ops[i][0] in (0, 2)) or (dev == 0 and ops[i][0] == 1))

        def feeds(i):
            return local(i) and i + 1 < len(ops) and ops[i + 1] == (ops[i][0] + 1, ops[i][1])

        row = []
        got = False
        seen_top = False
        for i in range(len(ops) + 1):
            e = 0
            if i < len(ops):
                kind, m = ops[i]
                e += KIND * kind + MB * m
                if got:
                    e += GOT
                got = False
                if i + 1 < len(ops):
                    nk, nm = ops[i + 1]
                    t0 = starts[dev][i][0]
                    arrive = starts[dev][i + 1][1]
                    own = dev == 0 and nk == 0
                    dependent = nm == m and nk == kind + 1
                    came_local = (dev == stages - 1 and nk in (1, 3)) or (dev == 0 and nk == 2)
                    prev_local = came_local and ops[i][1] == nm and ops[i][0] == nk - 1
                    if own or (not dependent and not prev_local and arrive + margin + (6.0 if nk < 2 else 0.0) <= t0):
                        e += PRE
                        got = True
                if kind in (1, 2) and not seen_top:
                    e += WW
                    seen_top = True
            if feeds(i - 1):
                e += WA
            elif local(i - 1):
                e += WB
            elif i == len(ops) and sends(i - 1):
                e += WB
            if sends(i - 2) and not local(i - 2):
                e += WC
            row.append(e)
        if len(row) % 2:
            row.append(0)
        rows.append([row[j] + ENTRY * row[j + 1] for j in range(0, len(row), 2)])
    return rows


def gelu_and_slope(a):
    a2 = a * a
    cdf = 0.5 * jnp.tanh(a * (K0 + (K0 * K1) * a2)) + 0.5
    u = a * cdf
    return u, cdf + (u * (1.0 - cdf)) * (2.0 * K0 + (6.0 * K0 * K1) * a2)


def pipeline_kernel(stages, table, seed_scale,
                    tokens, targets, w_in, w_out, gains,
                    xs, dhs, ns, us, gs, das, gain_sum, sse_sum,
                    wi, wo, xin, nx, ub, gt, ob, yt, sse_acc, sse_in,
                    recv_sem, half_sem, send_sem, in_sem, w_sem, out_sem, g_sem, x_sem, sse_send, sse_recv):
    me = lax.axis_index('stage')
    chunks = tokens.shape[0] // CHUNK
    d_model = tokens.shape[1]
    d_ff = w_in.shape[2]
    half = d_ff // HALVES
    first = me == 0
    last = me == stages - 1
    n_ops = 4 * chunks

    def weight_copies(row):
        copies = [pltpu.make_async_copy(w_in.at[row, :, pl.ds(h * half, half)], wi.at[row, h],
                                        w_sem.at[3 * row + h]) for h in range(HALVES)]
        return copies + [pltpu.make_async_copy(w_out.at[row], wo.at[row], w_sem.at[3 * row + HALVES])]

    for copy in weight_copies(0):
        copy.start()

    barrier = pltpu.get_barrier_semaphore()

    @pl.when(me > 0)
    def _():
        pl.semaphore_signal(barrier, inc=1, device_id={'stage': jnp.maximum(me - 1, 0)})

    @pl.when(me < stages - 1)
    def _():
        pl.semaphore_signal(barrier, inc=1, device_id={'stage': jnp.minimum(me + 1, stages - 1)})

    @pl.when(me > 1)
    def _():
        pl.semaphore_signal(barrier, inc=1, device_id={'stage': 0})

    @pl.when(first)
    def _():
        pl.semaphore_wait(barrier, stages - 1)

    @pl.when(last)
    def _():
        pl.semaphore_wait(barrier, 1)

    @pl.when(jnp.logical_not(first | last))
    def _():
        pl.semaphore_wait(barrier, 2)

    words = []
    for j in range(len(table[0])):
        word = jnp.int32(table[0][j])
        for dev in range(1, stages):
            word = jnp.where(me == dev, jnp.int32(table[dev][j]), word)
        words.append(word)

    def entry(s):
        word = words[0]
        pair = lax.div(s, 2)
        for j in range(1, len(words)):
            word = jnp.where(pair == j, words[j], word)
        return jnp.where(lax.rem(s, 2) == 0, lax.rem(word, ENTRY), lax.div(word, ENTRY))

    def flag(e, bit):
        return lax.rem(lax.div(e, bit), 2) == 1

    def fields(e):
        kind = lax.rem(e, 4)
        m = lax.rem(lax.div(e, MB), chunks)
        row = jnp.where((kind == 1) | (kind == 2), 1, 0)
        return kind, m, row

    def rows_of(m):
        return pl.ds(pl.multiple_of(m * CHUNK, CHUNK), CHUNK)

    def in_copy(slot):
        return pltpu.make_async_copy(tokens.at[pl.ds(0, CHUNK)], xin.at[slot], in_sem.at[slot])

    def sub_rows(m, sub):
        return pl.ds(pl.multiple_of(m * CHUNK + sub * SUB, SUB), SUB)

    def arrival(kind, m, row, sub):
        return pltpu.make_async_remote_copy(
            src_ref=ob.at[0, pl.ds(0, SUB)], dst_ref=xs.at[row, sub_rows(m, sub)], send_sem=send_sem.at[0],
            recv_sem=half_sem.at[(kind * chunks + m) * 2 + sub], device_id={'stage': me})

    def start_half(kind, m, row, slot, sub):
        from_tokens = (kind == 0) & first
        here = from_tokens | (last & (kind == 1))
        part = pl.ds(pl.multiple_of(sub * SUB, SUB), SUB)

        @pl.when(jnp.logical_not(here))
        def _():
            arrival(kind, m, row, sub).wait_recv()

        @pl.when(from_tokens)
        def _():
            pltpu.make_async_copy(tokens.at[sub_rows(m, sub)], xin.at[slot, part], in_sem.at[slot]).start()

        @pl.when(jnp.logical_not(from_tokens))
        def _():
            pltpu.make_async_copy(xs.at[row, sub_rows(m, sub)], xin.at[slot, part], in_sem.at[slot]).start()

        pltpu.make_async_copy(tokens.at[pl.ds(0, SUB)], xin.at[slot, part], in_sem.at[slot]).wait()

    def start_input(e, slot):
        kind, m, row = fields(e)
        rows = rows_of(m)
        here = (first & ((kind == 0) | (kind == 2))) | (last & ((kind == 1) | (kind == 3)))

        @pl.when(jnp.logical_not(here) & (kind < 2))
        def _():
            for sub in range(2):
                arrival(kind, m, row, sub).wait_recv()

        @pl.when(jnp.logical_not(here) & (kind >= 2))
        def _():
            pltpu.make_async_remote_copy(
                src_ref=ob.at[0], dst_ref=dhs.at[row, rows], send_sem=send_sem.at[0],
                recv_sem=recv_sem.at[kind * chunks + m], device_id={'stage': me}).wait_recv()

        @pl.when((kind == 0) & first)
        def _():
            pltpu.make_async_copy(tokens.at[rows], xin.at[slot], in_sem.at[slot]).start()

        @pl.when((kind < 2) & jnp.logical_not((kind == 0) & first))
        def _():
            pltpu.make_async_copy(xs.at[row, rows], xin.at[slot], in_sem.at[slot]).start()

        @pl.when(kind >= 2)
        def _():
            pltpu.make_async_copy(dhs.at[row, rows], xin.at[slot], in_sem.at[slot]).start()

    def sent(slot):
        return pltpu.make_async_copy(ob.at[slot], xs.at[0, pl.ds(0, CHUNK)], send_sem.at[slot])

    def slope_copy_in(row, rows, h):
        return pltpu.make_async_copy(gs.at[row, rows, pl.ds(h * half, half)], gt.at[h], g_sem.at[h])

    def start_slopes(e, halves):
        kind, m, row = fields(e)

        @pl.when(kind >= 2)
        def _():
            for h in halves:
                slope_copy_in(row, rows_of(m), h).start()

    def mid_step(e, e_next, slot, begin, end):
        @pl.when(begin & flag(e, WB))
        def _():
            sent(1 - slot).wait()

        @pl.when(begin & flag(e, WC))
        def _():
            sent(slot).wait()

        @pl.when(end & flag(e, PRE))
        def _():
            start_input(e_next, 1 - slot)

    gain_sum[...] = jnp.zeros_like(gain_sum)
    sse_acc[...] = jnp.zeros_like(sse_acc)
    for copy in weight_copies(0)[:HALVES]:
        copy.wait()

    def sse_copy(dev):
        return pltpu.make_async_remote_copy(
            src_ref=sse_sum, dst_ref=sse_in, send_sem=sse_send.at[dev], recv_sem=sse_recv,
            device_id={'stage': dev})

    BLK = 64

    def step(s, carry):
        e = entry(s)
        e_next = jnp.where(s + 1 < n_ops, entry(s + 1), 0)
        kind, m, row = fields(e)
        rows = rows_of(m)
        slot = lax.rem(s, 2)

        @pl.when(flag(e, WA))
        def _():
            sent(1 - slot).wait()

        @pl.when(jnp.logical_not(flag(e, GOT)) & (kind >= 2))
        def _():
            start_input(e, slot)

        @pl.when(flag(e, WW))
        def _():
            for copy in weight_copies(1):
                copy.wait()

        @pl.when(kind < 2)
        def _():
            @pl.when(flag(e, GOT))
            def _():
                in_copy(slot).wait()

            gain = gains[row]
            n_copy = pltpu.make_async_copy(nx, ns.at[row, rows], out_sem.at[0])
            g_copies = [pltpu.make_async_copy(gt.at[h], gs.at[row, rows, pl.ds(h * half, half)], g_sem.at[h])
                        for h in range(HALVES)]
            u_copies = [pltpu.make_async_copy(ub.at[h], us.at[row, rows, pl.ds(h * half, half)],
                                              out_sem.at[1 + h]) for h in range(HALVES)]

            @pl.loop(0, CHUNK // SUB)
            def _(sub):
                base = pl.multiple_of(sub * SUB, SUB)
                part = pl.ds(base, SUB)
                place = sub_rows(m, sub)

                @pl.when(jnp.logical_not(flag(e, GOT)))
                def _():
                    start_half(kind, m, row, slot, sub)

                @pl.loop(0, SUB // BLK)
                def _(b):
                    rb = pl.ds(pl.multiple_of(base + b * BLK, BLK), BLK)
                    x = xin[slot, rb].astype(F32)
                    inv = lax.rsqrt(jnp.mean(x * x, axis=-1, keepdims=True) + EPSILON)
                    nx[rb] = (x * inv * gain).astype(BF)

                pltpu.make_async_copy(nx.at[part], ns.at[row, place], out_sem.at[0]).start()
                for h in range(HALVES):
                    for j in range(half // 512):
                        a = jnp.dot(nx[part], wi[row, h, :, j * 512:(j + 1) * 512], preferred_element_type=F32)
                        for b in range(SUB // 16):
                            u, g = gelu_and_slope(a[b * 16:(b + 1) * 16])
                            rb = pl.ds(pl.multiple_of(base + b * 16, 16), 16)
                            ub[h, rb, j * 512:(j + 1) * 512] = u.astype(BF)
                            gt[h, rb, j * 512:(j + 1) * 512] = g
                    pltpu.make_async_copy(gt.at[h, part], gs.at[row, place, pl.ds(h * half, half)],
                                          g_sem.at[h]).start()
                    pltpu.make_async_copy(ub.at[h, part], us.at[row, place, pl.ds(h * half, half)],
                                          out_sem.at[1 + h]).start()

                @pl.when((s == 0) & (sub == 0))
                def _():
                    weight_copies(0)[HALVES].wait()
                    for copy in weight_copies(1):
                        copy.start()

                mid_step(e, e_next, slot, sub == 0, sub == 1)
                for j in range(d_model // 256 - 1):
                    cols = slice(j * 256, (j + 1) * 256)
                    y = jnp.dot(ub[0, part, :], wo[row, :half, cols], preferred_element_type=F32)
                    y += jnp.dot(ub[1, part, :], wo[row, half:, cols], preferred_element_type=F32)
                    ob[slot, part, cols] = (xin[slot, part, cols].astype(F32) + y).astype(BF)
                cols = slice(d_model - 256, d_model)
                yt[0] = jnp.dot(ub[0, part, :], wo[row, :half, cols], preferred_element_type=F32)
                yt[1] = jnp.dot(ub[1, part, :], wo[row, half:, cols], preferred_element_type=F32)
                ob[slot, part, cols] = (xin[slot, part, cols].astype(F32) + (yt[0] + yt[1])).astype(BF)

                @pl.when(first & (kind == 1))
                def _():
                    pltpu.make_async_copy(nx.at[part], ns.at[row, place], out_sem.at[0]).wait()
                    seed_copy = pltpu.make_async_copy(targets.at[place], nx.at[part], x_sem)
                    seed_copy.start()
                    seed_copy.wait()

                    @pl.loop(0, SUB // BLK)
                    def _(b):
                        rb = pl.ds(pl.multiple_of(base + b * BLK, BLK), BLK)
                        err = ob[slot, rb].astype(F32) - nx[rb].astype(F32)
                        ob[slot, rb] = (err * seed_scale).astype(BF)
                        sse_acc[...] += jnp.sum((err * err).reshape(BLK // 8, 8, d_model), axis=0)

                send_half(kind, m, row, slot, sub)

            @pl.when(jnp.logical_not(first & (kind == 1)))
            def _():
                n_copy.wait()

            for g_copy in g_copies:
                g_copy.wait()
            start_slopes(e_next, (0, 1))
            for u_copy in u_copies:
                u_copy.wait()

            @pl.when(first & (kind == 1) & (m == chunks - 1))
            def _():
                acc = sse_acc[:, :128]
                for j in range(1, d_model // 128):
                    acc += sse_acc[:, j * 128:(j + 1) * 128]
                sse_sum[...] = acc
                for dev in range(1, stages):
                    sse_copy(dev).start()

        @pl.when(kind >= 2)
        def _():
            @pl.when((kind == 3) & first)
            def _():
                pltpu.make_async_copy(tokens.at[rows], nx, x_sem).start()

            @pl.when(jnp.logical_not((kind == 3) & first))
            def _():
                pltpu.make_async_copy(xs.at[row, rows], nx, x_sem).start()

            in_copy(slot).wait()
            for h in range(HALVES):
                slope_copy_in(row, rows, h).wait()
                for j in range(half // 512):
                    lo = h * half + j * 512
                    du = lax.dot_general(xin[slot], wo[row, lo:lo + 512, :], NT, preferred_element_type=F32)
                    ub[h, :, j * 512:(j + 1) * 512] = (du * gt[h, :, j * 512:(j + 1) * 512]).astype(BF)
            da_copies = [pltpu.make_async_copy(ub.at[h], das.at[row, rows, pl.ds(h * half, half)],
                                               out_sem.at[1 + h]) for h in range(HALVES)]
            for da_copy in da_copies:
                da_copy.start()
            start_slopes(e_next, (0,))
            mid_step(e, e_next, slot, True, True)
            for j in range(d_model // 256 - 1):
                cols = slice(j * 256, (j + 1) * 256)
                gt[1, :, cols] = (
                    lax.dot_general(ub[0], wi[row, 0, cols, :], NT, preferred_element_type=F32)
                    + lax.dot_general(ub[1], wi[row, 1, cols, :], NT, preferred_element_type=F32))
            for h in range(HALVES):
                gt[1, :, d_model + (h - 1) * 256:d_model + h * 256] = lax.dot_general(
                    ub[h], wi[row, h, d_model - 256:, :], NT, preferred_element_type=F32)
            gt[1, :, d_model - 256:d_model] += gt[1, :, d_model:d_model + 256]
            pltpu.make_async_copy(tokens.at[pl.ds(0, CHUNK)], nx, x_sem).wait()
            gain = gains[row]

            @pl.loop(0, CHUNK // BLK)
            def _(b):
                rb = pl.ds(pl.multiple_of(b * BLK, BLK), BLK)
                x = nx[rb].astype(F32)
                inv = lax.rsqrt(jnp.mean(x * x, axis=-1, keepdims=True) + EPSILON)
                grad_n = gt[1, rb, :d_model]
                q = grad_n * gain
                proj = jnp.mean(q * x, axis=-1, keepdims=True)
                dx = q * inv - x * (inv * inv * inv * proj)
                ob[slot, rb] = (xin[slot, rb].astype(F32) + dx).astype(BF)
                gain_sum[row] += jnp.sum((grad_n * x * inv).reshape(BLK // 8, 8, d_model), axis=0)

            start_slopes(e_next, (1,))
            for da_copy in da_copies:
                da_copy.wait()
            send(kind, m, row, rows, slot)

        return carry

    def send(kind, m, row, rows, slot):
        down = (kind == 0) | (kind == 2)
        turn = (last & down) | (first & (kind == 1))
        stop = first & (kind == 3)
        to = jnp.where(down, jnp.minimum(me + 1, stages - 1), jnp.maximum(me - 1, 0))
        remote = jnp.logical_not(turn | stop)

        @pl.when(remote & (kind >= 2))
        def _():
            pltpu.make_async_remote_copy(
                src_ref=ob.at[slot], dst_ref=dhs.at[row, rows], send_sem=send_sem.at[slot],
                recv_sem=recv_sem.at[kind * chunks + m], device_id={'stage': to}).start()

        @pl.when(turn & (kind == 2))
        def _():
            pltpu.make_async_copy(ob.at[slot], dhs.at[0, rows], send_sem.at[slot]).start()

    def send_half(kind, m, row, slot, sub):
        down = kind == 0
        turn = (last & down) | (first & (kind == 1))
        to = jnp.where(down, jnp.minimum(me + 1, stages - 1), jnp.maximum(me - 1, 0))
        src = ob.at[slot, pl.ds(pl.multiple_of(sub * SUB, SUB), SUB)]
        place = sub_rows(m, sub)

        @pl.when(jnp.logical_not(turn))
        def _():
            pltpu.make_async_remote_copy(
                src_ref=src, dst_ref=xs.at[row, place], send_sem=send_sem.at[slot],
                recv_sem=half_sem.at[(kind * chunks + m) * 2 + sub], device_id={'stage': to}).start()

        @pl.when(turn & (kind == 0))
        def _():
            pltpu.make_async_copy(src, xs.at[1, place], send_sem.at[slot]).start()

        @pl.when(turn & (kind == 1))
        def _():
            pltpu.make_async_copy(src, dhs.at[1, place], send_sem.at[slot]).start()

    lax.fori_loop(0, n_ops, step, 0)
    e_end = entry(jnp.int32(n_ops))

    @pl.when(flag(e_end, WB))
    def _():
        sent((n_ops - 1) % 2).wait()

    @pl.when(flag(e_end, WC))
    def _():
        sent(n_ops % 2).wait()

    @pl.when(first)
    def _():
        for dev in range(1, stages):
            sse_copy(dev).wait_send()

    @pl.when(jnp.logical_not(first))
    def _():
        sse_copy(0).wait_recv()
        sse_sum[...] = sse_in[...]


def solution(mesh):
    stages = mesh.shape['stage']

    def device_step(tokens, targets, w_in, w_out, norm_gains):
        micro_count, tokens_mb, d_model = tokens.shape
        d_ff = w_in.shape[2]
        total = micro_count * tokens_mb
        chunks = total // CHUNK
        _, orders, starts = make_schedule(stages, chunks, 10.5, 9.5, 2.7, 9.5, 10.5)
        table = encode(stages, chunks, orders, starts, 2.0)
        any_spec = pl.BlockSpec(memory_space=pl.ANY)
        vmem_spec = pl.BlockSpec(memory_space=pltpu.VMEM)
        shape = jax.ShapeDtypeStruct
        xs, dhs, ns, us, gs, das, gain_sum, sse_sum = pl.pallas_call(
            functools.partial(pipeline_kernel, stages, table, 2.0 / total),
            out_shape=[shape((2, total, d_model), BF), shape((2, total, d_model), BF),
                       shape((2, total, d_model), BF), shape((2, total, d_ff), BF),
                       shape((2, total, d_ff), F32), shape((2, total, d_ff), BF),
                       shape((2, 8, d_model), F32), shape((8, 128), F32)],
            in_specs=[any_spec] * 4 + [vmem_spec],
            out_specs=[any_spec] * 6 + [vmem_spec] * 2,
            scratch_shapes=[
                pltpu.VMEM((2, HALVES, d_model, d_ff // HALVES), BF), pltpu.VMEM((2, d_ff, d_model), BF),
                pltpu.VMEM((2, CHUNK, d_model), BF), pltpu.VMEM((CHUNK, d_model), BF),
                pltpu.VMEM((HALVES, CHUNK, d_ff // HALVES), BF), pltpu.VMEM((HALVES, CHUNK, d_ff // HALVES), F32),
                pltpu.VMEM((2, CHUNK, d_model), BF), pltpu.VMEM((2, SUB, 256), F32),
                pltpu.VMEM((8, d_model), F32), pltpu.VMEM((8, 128), F32),
                pltpu.SemaphoreType.DMA((4 * chunks,)), pltpu.SemaphoreType.DMA((4 * chunks,)), pltpu.SemaphoreType.DMA((2,)),
                pltpu.SemaphoreType.DMA((2,)), pltpu.SemaphoreType.DMA((2 * HALVES + 2,)),
                pltpu.SemaphoreType.DMA((HALVES + 1,)), pltpu.SemaphoreType.DMA((HALVES,)),
                pltpu.SemaphoreType.DMA, pltpu.SemaphoreType.DMA((stages,)), pltpu.SemaphoreType.DMA,
            ],
            compiler_params=pltpu.CompilerParams(
                collective_id=0, has_side_effects=True, vmem_limit_bytes=67043328),
            name='vee',
        )(tokens.reshape(total, d_model), targets.reshape(total, d_model), w_in, w_out,
          norm_gains.reshape(2, 1, d_model))
        del xs, gs
        tok = (((1,), (1,)), ((0,), (0,)))
        grad_w_in = lax.dot_general(ns, das, tok, preferred_element_type=F32)
        grad_w_out = lax.dot_general(us, dhs, tok, preferred_element_type=F32)
        grad_gains = jnp.sum(gain_sum, axis=1)
        loss_value = jnp.sum(sse_sum) / (total * d_model)
        return grad_w_in, grad_w_out, grad_gains, loss_value.reshape(1)

    block_spec = P(('dp', 'stage'))
    return jax.shard_map(device_step, mesh=mesh,
                         in_specs=(P('dp'), P('dp'), P('stage'), P('stage'), P('stage')),
                         out_specs=(block_spec, block_spec, block_spec, P('dp')),
                         check_vma=False)
```
